256 devices in a mesh: gz: 16 (over z, y_lo), pa: 16 (over y_hi, x, core).
Axes of the slice: x: 4, y: 4 (y_hi: 2, y_lo: 2; y = y_hi * 2 + y_lo), z: 8, core: 2. Of those that a mesh axis runs over, the one named last changes fastest.
Arguments:
- density: bfloat16 [64, 1024, 1024], P('gz', 'pa'), may hold values from -6 to 6
- green: float32 [128, 1024, 1024], P('gz', 'pa'), may hold values from 0.1 to 3
Outputs:
- potential: float32 [64, 1024, 1024], P('gz', 'pa')
The draws below stay inside these ranges and needn't reach their ends.
All inputs are finite; a program needn't handle non-finite values.
Results may differ from the reference program's by a relative error of at most 0.02.
Values may be sent and summed in bfloat16 or wider, within the bound.
A program may use at most 64 MiB of HBM per device.

```python
import math
import jax
import jax.numpy as jnp
from jax import lax

NX = 1024
NY = 1024
NZ = 64
M = 128
N_GZ = 16


def level_of(key, dims, cuts, least, high):
    level = 1.0
    for axis_at, shards_of in cuts:
        steps = jax.random.uniform(jax.random.fold_in(jax.random.fold_in(key, 6), axis_at), (shards_of,), jnp.float32, least / len(cuts), high / len(cuts))
        level = level * jnp.repeat(jnp.exp(steps), dims[axis_at] // shards_of).reshape((-1,) + (1,) * (len(dims) - 1 - axis_at))
    return level


def scatter_about(stream_key, extent, deviation, limit, cuts=(), kind=jnp.bfloat16):
    drawn = jax.random.normal(stream_key, extent, jnp.float32) * deviation
    if len(cuts) > 0:
        drawn = level_of(stream_key, extent, cuts, -0.22, 0.18) * drawn
    return jnp.clip(drawn, min=-limit, max=limit).astype(kind)


def setup_inputs(seed: int = 0) -> dict:
    arg_keys = jax.random.split(jax.random.key(seed), 3)
    return {
        "density": scatter_about(arg_keys[0], (NZ, NX, NY), 1.0, 6.0, ((0, 16), (1, 16))),
        "green": jnp.clip(jnp.exp(math.log(3.0) - 3.4011974 * jax.random.uniform(arg_keys[1], (M, NY, NX), jnp.float32) ** level_of(arg_keys[1], (M, NY, NX), ((0, 16), (1, 16)), -0.2, 0.2)), 0.1, 3.0),
    }


def cas_table(rows, cols, length):
    product = (rows[:, None] * cols[None, :]) % length
    angle = product.astype(jnp.float32) * (2.0 * math.pi / length)
    return (jnp.cos(angle) + jnp.sin(angle)).astype(jnp.bfloat16)


def blocked_sum(tables, pieces, rows, columns):
    def add_block(total, pair):
        table, piece = pair
        term = jnp.dot(table, piece, precision=lax.Precision.HIGHEST, preferred_element_type=jnp.float32).astype(jnp.bfloat16)
        term = lax.optimization_barrier(term)
        return total + term.astype(jnp.float32), None

    total, _ = lax.scan(add_block, jnp.zeros((rows, columns), jnp.float32), (tables, pieces))
    return total


def reference(density, green):
    z_cells, x_cells, y_cells = density.shape
    z_freqs = 2 * z_cells
    z_slab = z_cells // N_GZ
    k_block = z_freqs // N_GZ
    columns = x_cells * y_cells
    highest = lax.Precision.HIGHEST
    f_index = jnp.arange(z_freqs, dtype=jnp.int32)
    z_index = jnp.arange(z_cells, dtype=jnp.int32)
    forward_tables = cas_table(f_index, z_index, z_freqs).astype(jnp.float32).reshape(z_freqs, N_GZ, z_slab).transpose(1, 0, 2)
    slabs = density.astype(jnp.float32).reshape(N_GZ, z_slab, columns)
    zspec = blocked_sum(forward_tables, slabs, z_freqs, columns).astype(jnp.bfloat16).reshape(z_freqs, x_cells, y_cells)
    cas_y = cas_table(jnp.arange(y_cells, dtype=jnp.int32), jnp.arange(y_cells, dtype=jnp.int32), y_cells).astype(jnp.float32)
    cas_x = cas_table(jnp.arange(x_cells, dtype=jnp.int32), jnp.arange(x_cells, dtype=jnp.int32), x_cells).astype(jnp.float32)
    yspec = jnp.einsum('kxy,vy->kxv', zspec.astype(jnp.float32), cas_y, precision=highest).astype(jnp.bfloat16)
    xspec = jnp.einsum('kxv,ux->kvu', yspec.astype(jnp.float32), cas_x, precision=highest)
    weighted = (green * xspec).astype(jnp.bfloat16)
    yback = jnp.einsum('kvu,xu->kxv', weighted.astype(jnp.float32), cas_x, precision=highest).astype(jnp.bfloat16)
    zback = jnp.einsum('kxv,yv->kxy', yback.astype(jnp.float32), cas_y, precision=highest).astype(jnp.bfloat16)
    back_tables = cas_table(z_index, f_index, z_freqs).astype(jnp.float32).reshape(z_cells, N_GZ, k_block).transpose(1, 0, 2)
    blocks = zback.astype(jnp.float32).reshape(N_GZ, k_block, columns)
    total = blocked_sum(back_tables, blocks, z_cells, columns)
    scale = 1.0 / (x_cells * y_cells * z_freqs)
    return (total * scale).reshape(z_cells, x_cells, y_cells)
```

```python
import math

import jax
import jax.numpy as jnp
import numpy as np
from jax import lax
from jax.sharding import PartitionSpec as P


def cas_table(rows, cols, length):
    product = np.arange(rows)[:, None] * np.arange(cols)[None, :] % length
    angle = product.astype(np.float32) * np.float32(2.0 * math.pi / length)
    return jnp.asarray((np.cos(angle) + np.sin(angle)).astype(np.float32), jnp.bfloat16)


def dot(spec, a, b):
    return jnp.einsum(spec, a, b, preferred_element_type=jnp.float32)


def exchange(value, axis):
    return lax.all_to_all(value, axis, split_axis=0, concat_axis=0, tiled=True)


def local(density, green, cas, cas_z):
    z_slab, x_local, y_cells = density.shape
    k_block, y_local, x_cells = green.shape
    groups = lax.axis_size("gz")
    pencils = lax.axis_size("pa")
    z_freqs = k_block * groups
    z_cells = z_slab * groups
    u_local = x_cells // groups
    half = jnp.bfloat16

    moved_green = green.astype(half).reshape(k_block, y_local, groups, u_local)
    moved_green = moved_green.transpose(2, 0, 1, 3).reshape(groups * k_block, y_local * u_local)
    moved_green = exchange(moved_green, "gz")

    yspec = dot("zxy,vy->vzx", density, cas).astype(half)
    yspec = exchange(yspec.reshape(y_cells, z_slab * x_local), "pa")
    yspec = yspec.reshape(pencils, y_local, z_slab, x_local)
    spectrum = dot("qvzl,uql->zvu", yspec, cas.reshape(x_cells, pencils, x_local)).astype(half)
    spectrum = spectrum.reshape(z_slab, y_local, groups, u_local).transpose(2, 0, 1, 3)
    spectrum = exchange(spectrum.reshape(groups * z_slab, y_local * u_local), "gz")
    spectrum = dot("kz,zs->ks", cas_z, spectrum)
    weighted = (moved_green.astype(jnp.float32) * spectrum).astype(half)
    back = dot("kz,ks->zs", cas_z, weighted).astype(half)
    back = exchange(back, "gz").reshape(groups, z_slab, y_local, u_local)
    back = dot("gzvu,xgu->xzv", back, cas.reshape(x_cells, groups, u_local)).astype(half)
    back = exchange(back.reshape(x_cells, z_slab * y_local), "pa")
    back = back.reshape(pencils, x_local, z_slab, y_local)
    total = dot("qlzv,yqv->zly", back, cas.reshape(y_cells, pencils, y_local))
    return total * (1.0 / (x_cells * y_cells * z_freqs))


def solution(mesh):
    cas = cas_table(1024, 1024, 1024)
    cas_z = cas_table(128, 64, 128)
    step = jax.shard_map(
        local,
        mesh=mesh,
        in_specs=(P("gz", "pa", None), P("gz", "pa", None), P(), P()),
        out_specs=P("gz", "pa", None),
        check_vma=False,
    )
    return lambda density, green: step(density, green, cas, cas_z)
```

```python
import math

import jax
import jax.numpy as jnp
import numpy as np
from jax import lax
from jax.experimental import pallas as pl
from jax.experimental.pallas import tpu as pltpu
from jax.sharding import PartitionSpec as P

MESH = pl.DeviceIdType.MESH
HALF = jnp.bfloat16
N = 16


def cas_table(rows, cols, length):
    product = np.arange(rows)[:, None] * np.arange(cols)[None, :] % length
    angle = product.astype(np.float32) * np.float32(2.0 * math.pi / length)
    return jnp.asarray((np.cos(angle) + np.sin(angle)).astype(np.float32), HALF)


def dot(a, b):
    return jnp.dot(a, b, preferred_element_type=jnp.float32)


def dot_nt(a, b):
    return lax.dot_general(a, b, (((1,), (1,)), ((), ())), preferred_element_type=jnp.float32)


def iota(shape, dim):
    return lax.broadcasted_iota(jnp.int32, shape, dim)


def block(index, size):
    return pl.ds(pl.multiple_of(index * size, size), size)


def kernel(
    scale,
    density_hbm,
    green_hbm,
    cas_hbm,
    casz_ref,
    caszt_ref,
    out_ref,
    rhs,
    green_in,
    cas,
    cas2,
    kron_f,
    kron_i,
    green_out,
    green_all,
    y_out,
    y_all,
    lhs,
    x_out,
    x_all,
    z_in,
    z_mid,
    z_out,
    z_all,
    i_out,
    i_all,
    load_sem,
    send_sem,
    recv_sem,
):
    me_g = lax.axis_index("gz")
    me_p = lax.axis_index("pa")
    me = {"gz": me_g, "pa": me_p}

    loads = [
        pltpu.make_async_copy(source, target, load_sem.at[i])
        for i, (source, target) in enumerate(
            ((cas_hbm, cas), (density_hbm, rhs), (green_hbm, green_in))
        )
    ]
    for load in loads:
        load.start()

    barrier = pltpu.get_barrier_semaphore()
    for axis in ("gz", "pa"):

        @pl.loop(1, N)
        def _(s, axis=axis):
            pl.semaphore_signal(
                barrier, inc=1, device_id={axis: lax.rem(me[axis] + s, N)}, device_id_type=MESH
            )

    def copy(which, axis, source, target, peer):
        s = lax.rem(peer - me[axis] + N, N)
        return pltpu.make_async_remote_copy(
            src_ref=source.at[peer],
            dst_ref=target.at[me[axis]],
            send_sem=send_sem.at[which, s],
            recv_sem=recv_sem.at[which, s],
            device_id={axis: peer},
            device_id_type=MESH,
        )

    def send(which, axis, source, target, peer):
        @pl.when(peer != me[axis])
        def _():
            copy(which, axis, source, target, peer).start()

        @pl.when(peer == me[axis])
        def _():
            target[me[axis]] = source[me[axis]]

    def send_all(which, axis, source, target):
        @pl.loop(0, N)
        def _(i):
            far = jnp.where(lax.rem(i, 2) == 0, N // 2 + i // 2, N // 2 - (i + 1) // 2)
            send(which, axis, source, target, lax.rem(me[axis] + far, N))

    def receive(which, axis, source, target):
        @pl.loop(1, N)
        def _(s):
            copy(which, axis, source, target, lax.rem(me[axis] + s, N)).wait_recv()

    def drain(which, axis, source, target):
        @pl.loop(1, N)
        def _(s):
            copy(which, axis, source, target, lax.rem(me[axis] + s, N)).wait_send()

    loads[0].wait()
    loads[1].wait()

    @pl.loop(0, 4)
    def _(j):
        value = dot_nt(cas[block(j, 256), :], rhs[...]).astype(HALF)
        for i in range(4):
            y_out[4 * j + i] = value[64 * i : 64 * (i + 1), :]

    loads[2].wait()

    @pl.loop(0, 8)
    def _(k):
        for b in range(8):
            value = green_in[k, :, 128 * b : 128 * (b + 1)].astype(HALF)
            green_out[2 * b, k] = value[:32]
            green_out[2 * b + 1, k] = value[32:]

    pl.semaphore_wait(barrier, 2 * (N - 1))
    send_all(0, "pa", y_out, y_all)
    send_all(1, "gz", green_out, green_all)

    @pl.loop(0, N)
    def _(q):
        value = cas[block(q, 64), :]
        cas2[block(2 * q, 64), :] = value
        cas2[block(2 * q + 1, 64), :] = value

    def spread(table, target, rows, cols):
        @pl.loop(0, rows // 16)
        def _(j):
            pick = (iota((128, rows), 0) >> 3) + 16 * j == iota((128, rows), 1)
            part = dot(pick.astype(jnp.float32).astype(HALF), table[...]).astype(HALF)
            wide = (iota((cols, 8 * cols), 1) >> 3) == iota((cols, 8 * cols), 0)
            full = dot(part, wide.astype(jnp.float32).astype(HALF))
            same = (iota((128, 8 * cols), 0) & 7) == (iota((128, 8 * cols), 1) & 7)
            target[block(j, 128), :] = jnp.where(same, full, 0.0).astype(HALF)

    spread(casz_ref, kron_f, 128, 64)
    spread(caszt_ref, kron_i, 64, 128)

    low = (iota((64, 128), 1) < 64).astype(jnp.float32).astype(HALF)
    masks = (low, (1.0 - low.astype(jnp.float32)).astype(HALF))

    def spread_planes(source):
        @pl.loop(0, N)
        def _(q):
            for z in range(4):
                part = source[q, :, 128 * (z // 2) : 128 * (z // 2 + 1)]
                lhs[64 * z : 64 * (z + 1), block(q, 128)] = part * masks[z % 2]

    receive(0, "pa", y_out, y_all)
    spread_planes(y_all)

    @pl.loop(0, 4)
    def _(i):
        j = lax.rem(i + me_g // 4 + 1, 4)
        value = dot(lhs[...], cas2[:, block(j, 256)]).astype(HALF)
        for u in range(2):
            for v in range(2):
                for z in range(4):
                    row = 64 * z + 32 * v
                    x_out[4 * j + 2 * u + v, z] = value[row : row + 32, 128 * u : 128 * (u + 1)]
        for b in range(4):
            send(2, "gz", x_out, x_all, 4 * j + b)

    receive(2, "gz", x_out, x_all)
    receive(1, "gz", green_out, green_all)

    for h in range(2):
        rows = slice(16 * h, 16 * h + 16)

        @pl.loop(0, N)
        def _(g):
            value = x_all[g, :, rows, :].astype(jnp.float32)
            for v in range(2):
                part = value[:, 8 * v : 8 * v + 8, :].reshape(32, 128)
                z_in[block(g, 32), 128 * v : 128 * (v + 1)] = part.astype(HALF)

        @pl.loop(0, 4)
        def _(j):
            value = dot(kron_f[block(j, 256), :], z_in[...])
            for i in range(4):
                weight = green_all[4 * j + i, :, rows, :].astype(jnp.float32)
                for v in range(2):
                    part = weight[:, 8 * v : 8 * v + 8, :].reshape(64, 128)
                    part = part * value[64 * i : 64 * i + 64, 128 * v : 128 * (v + 1)]
                    z_mid[pl.ds(pl.multiple_of(256 * j + 64 * i, 64), 64), 128 * v : 128 * (v + 1)] = part.astype(HALF)

        @pl.loop(0, 2)
        def _(j):
            value = dot(kron_i[block(j, 256), :], z_mid[...])
            for i in range(8):
                part = value[32 * i : 32 * i + 32]
                part = jnp.concatenate(
                    [part[:, 128 * v : 128 * (v + 1)].reshape(4, 8, 128) for v in range(2)], axis=1
                )
                z_out[8 * j + i, :, rows, :] = part.astype(HALF)

    send_all(3, "gz", z_out, z_all)
    receive(3, "gz", z_out, z_all)

    @pl.loop(0, 8)
    def _(u):
        for v in range(2):
            for z in range(4):
                row = 64 * z + 32 * v
                rhs[row : row + 32, block(u, 128)] = z_all[2 * u + v, z]

    @pl.loop(0, 4)
    def _(i):
        j = lax.rem(i + me_p // 4 + 1, 4)
        value = dot_nt(cas[block(j, 256), :], rhs[...]).astype(HALF)
        for b in range(4):
            i_out[4 * j + b] = value[64 * b : 64 * (b + 1), :]
            send(4, "pa", i_out, i_all, 4 * j + b)

    receive(4, "pa", i_out, i_all)
    spread_planes(i_all)

    @pl.loop(0, 4)
    def _(j):
        out_ref[:, block(j, 256)] = dot(lhs[...], cas2[:, block(j, 256)]) * scale

    drain(0, "pa", y_out, y_all)
    drain(1, "gz", green_out, green_all)
    drain(2, "gz", x_out, x_all)
    drain(3, "gz", z_out, z_all)
    drain(4, "pa", i_out, i_all)


def solution(mesh):
    cas = cas_table(1024, 1024, 1024)
    cas_z = cas_table(128, 64, 128)
    cas_zt = cas_table(64, 128, 128)
    scale = 1.0 / (1024 * 1024 * 128)

    def local(density, green, cas, cas_z, cas_zt):
        def vmem(*shape, dtype=HALF):
            return pltpu.VMEM(shape, dtype)

        anywhere = pl.BlockSpec(memory_space=pl.ANY)
        near = pl.BlockSpec(memory_space=pltpu.VMEM)
        potential = pl.pallas_call(
            lambda *refs: kernel(scale, *refs),
            out_shape=jax.ShapeDtypeStruct((256, 1024), jnp.float32),
            in_specs=[anywhere, anywhere, anywhere, near, near],
            out_specs=near,
            scratch_shapes=[
                vmem(256, 1024),
                vmem(8, 64, 1024, dtype=jnp.float32),
                vmem(1024, 1024),
                vmem(2048, 1024),
                vmem(1024, 512),
                vmem(512, 1024),
                vmem(N, 8, 32, 128),
                vmem(N, 8, 32, 128),
                vmem(N, 64, 256),
                vmem(N, 64, 256),
                vmem(256, 2048),
                vmem(N, 4, 32, 128),
                vmem(N, 4, 32, 128),
                vmem(512, 256),
                vmem(1024, 256),
                vmem(N, 4, 32, 128),
                vmem(N, 4, 32, 128),
                vmem(N, 64, 256),
                vmem(N, 64, 256),
                pltpu.SemaphoreType.DMA((3,)),
                pltpu.SemaphoreType.DMA((5, N)),
                pltpu.SemaphoreType.DMA((5, N)),
            ],
            compiler_params=pltpu.CompilerParams(
                collective_id=0, has_side_effects=True, vmem_limit_bytes=60 * 1024 * 1024
            ),
            name="poisson",
        )(density.reshape(256, 1024), green, cas, cas_z, cas_zt)
        return potential.reshape(4, 64, 1024)

    step = jax.shard_map(
        local,
        mesh=mesh,
        in_specs=(P("gz", "pa", None), P("gz", "pa", None), P(), P(), P()),
        out_specs=P("gz", "pa", None),
        check_vma=False,
    )
    return lambda density, green: step(density, green, cas, cas_z, cas_zt)
```

```python
import math

import jax
import jax.numpy as jnp
import numpy as np
from jax import lax
from jax.experimental import pallas as pl
from jax.experimental.pallas import tpu as pltpu
from jax.sharding import PartitionSpec as P

MESH = pl.DeviceIdType.MESH
HALF = jnp.bfloat16
N = 16
PARTS = 2


def cas_table(rows, cols, length):
    product = np.arange(rows)[:, None] * np.arange(cols)[None, :] % length
    angle = product.astype(np.float32) * np.float32(2.0 * math.pi / length)
    return jnp.asarray((np.cos(angle) + np.sin(angle)).astype(np.float32), HALF)


def dot(a, b):
    return jnp.dot(a, b, preferred_element_type=jnp.float32)


def dot_nt(a, b):
    return lax.dot_general(a, b, (((1,), (1,)), ((), ())), preferred_element_type=jnp.float32)


def iota(shape, dim):
    return lax.broadcasted_iota(jnp.int32, shape, dim)


def one_hot(condition):
    return condition.astype(jnp.float32).astype(HALF)


def block(index, size):
    return pl.ds(pl.multiple_of(index * size, size), size)


def kernel(
    scale,
    density_hbm,
    green_hbm,
    cas_hbm,
    casz_ref,
    caszt_ref,
    out_ref,
    planes,
    green_in,
    cas,
    cas2,
    cas4,
    kron_f,
    kron_i,
    green_out,
    green_all,
    y_out,
    y_all,
    lhs_x,
    x_out,
    x_all,
    z_in,
    z_mid,
    z_out,
    z_all,
    rhs,
    i_out,
    i_all,
    lhs_y,
    load_sem,
    send_sem,
    recv_sem,
):
    me = {"gz": lax.axis_index("gz"), "pa": lax.axis_index("pa")}

    loads = [
        pltpu.make_async_copy(source, target, load_sem.at[i])
        for i, (source, target) in enumerate(
            ((cas_hbm, cas), (density_hbm, planes), (green_hbm, green_in))
        )
    ]
    for load in loads:
        load.start()

    barrier = pltpu.get_barrier_semaphore()
    for axis in ("gz", "pa"):

        @pl.loop(1, N)
        def _(s, axis=axis):
            pl.semaphore_signal(
                barrier, inc=1, device_id={axis: lax.rem(me[axis] + s, N)}, device_id_type=MESH
            )

    class Exchange:
        def __init__(self, number, axis, source, target):
            self.number, self.axis, self.source, self.target = number, axis, source, target

        def copy(self, peer):
            mine = me[self.axis]
            s = lax.rem(peer - mine + N, N)
            return pltpu.make_async_remote_copy(
                src_ref=self.source.at[peer],
                dst_ref=self.target.at[mine],
                send_sem=send_sem.at[self.number, s],
                recv_sem=recv_sem.at[self.number, s],
                device_id={self.axis: peer},
                device_id_type=MESH,
            )

        def send(self, peer):
            mine = me[self.axis]

            @pl.when(peer != mine)
            def _():
                self.copy(peer).start()

            @pl.when(peer == mine)
            def _():
                self.target[mine] = self.source[mine]

        def send_all(self):
            @pl.loop(0, N)
            def _(i):
                far = jnp.where(lax.rem(i, 2) == 0, N // 2 + i // 2, N // 2 - (i + 1) // 2)
                self.send(lax.rem(me[self.axis] + far, N))

        def receive(self):
            @pl.loop(1, N)
            def _(s):
                self.copy(lax.rem(me[self.axis] + s, N)).wait_recv()

        def drain(self):
            @pl.loop(1, N)
            def _(s):
                self.copy(lax.rem(me[self.axis] + s, N)).wait_send()

    ex_y = Exchange(0, "pa", y_out, y_all)
    ex_green = [Exchange(1 + h, "gz", green_out.at[h], green_all.at[h]) for h in range(PARTS)]
    ex_x = [Exchange(3 + h, "gz", x_out.at[h], x_all.at[h]) for h in range(PARTS)]
    ex_z = [Exchange(5 + h, "gz", z_out.at[h], z_all.at[h]) for h in range(PARTS)]
    ex_i = [Exchange(7 + h, "pa", i_out.at[h], i_all.at[h]) for h in range(PARTS)]

    def y_forward():
        @pl.loop(0, 4)
        def _(j):
            value = dot_nt(cas[block(j, 256), :], planes[...]).astype(HALF)
            for i in range(4):
                y_out[4 * j + i] = value[64 * i : 64 * (i + 1), :]

    def green_narrow():
        @pl.loop(0, 8)
        def _(k):
            for u in range(8):
                value = green_in[k, :, 128 * u : 128 * (u + 1)].astype(HALF)
                for v in range(2):
                    for h in range(PARTS):
                        row = 32 * v + 16 * h
                        green_out[h, 2 * u + v, k] = value[row : row + 16]

    def tables():
        @pl.loop(0, N)
        def _(q):
            value = cas[block(q, 64), :]
            cas2[block(2 * q, 64), :] = value
            cas2[block(2 * q + 1, 64), :] = value
            for h in range(PARTS):
                for z in range(4):
                    for v in range(2):
                        row = 32 * v + 16 * h
                        cas4[h, block(q * 8 + z * 2 + v, 16), :] = value[row : row + 16]

        def spread(table, target, rows, cols):
            @pl.loop(0, rows // 16)
            def _(j):
                pick = (iota((128, rows), 0) >> 3) + 16 * j == iota((128, rows), 1)
                part = dot(one_hot(pick), table[...]).astype(HALF)
                wide = (iota((cols, 8 * cols), 1) >> 3) == iota((cols, 8 * cols), 0)
                full = dot(part, one_hot(wide))
                same = (iota((128, 8 * cols), 0) & 7) == (iota((128, 8 * cols), 1) & 7)
                target[block(j, 128), :] = jnp.where(same, full, 0.0).astype(HALF)

        spread(casz_ref, kron_f, 128, 64)
        spread(caszt_ref, kron_i, 64, 128)

    lane = iota((64, 128), 1)

    def x_operand():
        masks = [one_hot((lane >> 6) == z) for z in range(2)]

        @pl.loop(0, N)
        def _(q):
            for z in range(4):
                part = y_all[q, :, 128 * (z // 2) : 128 * (z // 2 + 1)] * masks[z % 2]
                for h in range(PARTS):
                    for v in range(2):
                        row = 32 * v + 16 * h
                        to = 128 * h + 32 * z + 16 * v
                        lhs_x[to : to + 16, block(q, 128)] = part[row : row + 16]

    def x_forward(h):
        @pl.loop(0, 4)
        def _(i):
            j = lax.rem(i + me["gz"] // 4 + 1, 4)
            value = dot(lhs_x[128 * h : 128 * (h + 1), :], cas2[:, block(j, 256)]).astype(HALF)
            for u in range(2):
                for v in range(2):
                    for z in range(4):
                        row = 32 * z + 16 * v
                        x_out[h, 4 * j + 2 * u + v, z] = value[
                            row : row + 16, 128 * u : 128 * (u + 1)
                        ]
            for b in range(4):
                ex_x[h].send(4 * j + b)

    def z_both(h):
        @pl.loop(0, N)
        def _(g):
            value = x_all[h, g].astype(jnp.float32)
            for v in range(2):
                part = value[:, 8 * v : 8 * v + 8, :].reshape(32, 128)
                z_in[block(g, 32), 128 * v : 128 * (v + 1)] = part.astype(HALF)

        @pl.loop(0, 4)
        def _(j):
            value = dot(kron_f[block(j, 256), :], z_in[...])
            for i in range(4):
                weight = green_all[h, 4 * j + i].astype(jnp.float32)
                for v in range(2):
                    part = weight[:, 8 * v : 8 * v + 8, :].reshape(64, 128)
                    part = part * value[64 * i : 64 * i + 64, 128 * v : 128 * (v + 1)]
                    z_mid[block(4 * j + i, 64), 128 * v : 128 * (v + 1)] = part.astype(HALF)

        @pl.loop(0, 2)
        def _(i):
            j = lax.rem(i + me["gz"] // 8 + 1, 2)
            value = dot(kron_i[block(j, 256), :], z_mid[...])
            for b in range(8):
                part = value[32 * b : 32 * b + 32]
                part = jnp.concatenate(
                    [part[:, 128 * v : 128 * (v + 1)].reshape(4, 8, 128) for v in range(2)], axis=1
                )
                z_out[h, 8 * j + b] = part.astype(HALF)
            for b in range(8):
                ex_z[h].send(8 * j + b)

    def x_inverse(h):
        @pl.loop(0, 8)
        def _(u):
            for v in range(2):
                for z in range(4):
                    row = 32 * z + 16 * v
                    rhs[row : row + 16, block(u, 128)] = z_all[h, 2 * u + v, z]

        @pl.loop(0, 4)
        def _(i):
            j = lax.rem(i + me["pa"] // 4 + 1, 4)
            value = dot_nt(cas[block(j, 256), :], rhs[...]).astype(HALF)
            for b in range(4):
                i_out[h, 4 * j + b] = value[64 * b : 64 * (b + 1), :]
            for b in range(4):
                ex_i[h].send(4 * j + b)

    def y_inverse(h):
        masks = [one_hot((lane >> 5) == z) for z in range(4)]

        @pl.loop(0, N)
        def _(q):
            value = i_all[h, q]
            for z in range(4):
                lhs_y[64 * z : 64 * (z + 1), block(q, 128)] = value * masks[z]

        @pl.loop(0, 4)
        def _(j):
            value = dot(lhs_y[...], cas4[h, :, block(j, 256)])
            if h == 0:
                out_ref[:, block(j, 256)] = value
            else:
                out_ref[:, block(j, 256)] = (out_ref[:, block(j, 256)] + value) * scale

    scope = jax.named_scope
    with scope("load"):
        loads[0].wait()
        loads[1].wait()
    with scope("y_forward"):
        y_forward()
    with scope("green_narrow"):
        loads[2].wait()
        green_narrow()
    with scope("barrier"):
        pl.semaphore_wait(barrier, 2 * (N - 1))
    with scope("send_y"):
        ex_y.send_all()
        ex_green[0].send_all()
    with scope("tables"):
        tables()
    with scope("wait_y"):
        ex_y.receive()
    with scope("x_operand"):
        x_operand()
    with scope("x_forward0"):
        x_forward(0)
    with scope("send_green1"):
        ex_green[1].send_all()
    with scope("x_forward1"):
        x_forward(1)
    for h in range(PARTS):
        with scope(f"wait_green{h}"):
            ex_green[h].receive()
        with scope(f"wait_x{h}"):
            ex_x[h].receive()
        with scope(f"z_both{h}"):
            z_both(h)
    for h in range(PARTS):
        with scope(f"wait_z{h}"):
            ex_z[h].receive()
        with scope(f"x_inverse{h}"):
            x_inverse(h)
    for h in range(PARTS):
        with scope(f"wait_i{h}"):
            ex_i[h].receive()
        with scope(f"y_inverse{h}"):
            y_inverse(h)
    with scope("drain"):
        for exchange in [ex_y, *ex_green, *ex_x, *ex_z, *ex_i]:
            exchange.drain()


def solution(mesh):
    cas = cas_table(1024, 1024, 1024)
    cas_z = cas_table(128, 64, 128)
    cas_zt = cas_table(64, 128, 128)
    scale = 1.0 / (1024 * 1024 * 128)

    def local(density, green, cas, cas_z, cas_zt):
        def vmem(*shape, dtype=HALF):
            return pltpu.VMEM(shape, dtype)

        anywhere = pl.BlockSpec(memory_space=pl.ANY)
        near = pl.BlockSpec(memory_space=pltpu.VMEM)
        potential = pl.pallas_call(
            lambda *refs: kernel(scale, *refs),
            out_shape=jax.ShapeDtypeStruct((256, 1024), jnp.float32),
            in_specs=[anywhere, anywhere, anywhere, near, near],
            out_specs=near,
            scratch_shapes=[
                vmem(256, 1024),
                vmem(8, 64, 1024, dtype=jnp.float32),
                vmem(1024, 1024),
                vmem(2048, 1024),
                vmem(PARTS, 2048, 1024),
                vmem(1024, 512),
                vmem(512, 1024),
                vmem(PARTS, N, 8, 16, 128),
                vmem(PARTS, N, 8, 16, 128),
                vmem(N, 64, 256),
                vmem(N, 64, 256),
                vmem(256, 2048),
                vmem(PARTS, N, 4, 16, 128),
                vmem(PARTS, N, 4, 16, 128),
                vmem(512, 256),
                vmem(1024, 256),
                vmem(PARTS, N, 4, 16, 128),
                vmem(PARTS, N, 4, 16, 128),
                vmem(128, 1024),
                vmem(PARTS, N, 64, 128),
                vmem(PARTS, N, 64, 128),
                vmem(256, 2048),
                pltpu.SemaphoreType.DMA((3,)),
                pltpu.SemaphoreType.DMA((9, N)),
                pltpu.SemaphoreType.DMA((9, N)),
            ],
            compiler_params=pltpu.CompilerParams(
                collective_id=0, has_side_effects=True, vmem_limit_bytes=60 * 1024 * 1024
            ),
            name="poisson",
        )(density.reshape(256, 1024), green, cas, cas_z, cas_zt)
        return potential.reshape(4, 64, 1024)

    step = jax.shard_map(
        local,
        mesh=mesh,
        in_specs=(P("gz", "pa", None), P("gz", "pa", None), P(), P(), P()),
        out_specs=P("gz", "pa", None),
        check_vma=False,
    )
    return lambda density, green: step(density, green, cas, cas_z, cas_zt)
```

```python
import math

import jax
import jax.numpy as jnp
import numpy as np
from jax import lax
from jax.experimental import pallas as pl
from jax.experimental.pallas import tpu as pltpu
from jax.sharding import PartitionSpec as P

MESH = pl.DeviceIdType.MESH
HALF = jnp.bfloat16
N = 16
PARTS = 2
FAR_FIRST = [8, 7, 9, 6, 10, 5, 11, 4, 12, 3, 13, 2, 14, 1, 15]


def cas_table(rows, cols, length):
    product = np.arange(rows)[:, None] * np.arange(cols)[None, :] % length
    angle = product.astype(np.float32) * np.float32(2.0 * math.pi / length)
    return jnp.asarray((np.cos(angle) + np.sin(angle)).astype(np.float32), HALF)


def dot(a, b):
    return jnp.dot(a, b, preferred_element_type=jnp.float32)


def dot_nt(a, b):
    return lax.dot_general(a, b, (((1,), (1,)), ((), ())), preferred_element_type=jnp.float32)


def iota(shape, dim):
    return lax.broadcasted_iota(jnp.int32, shape, dim)


def one_hot(condition):
    return condition.astype(jnp.float32).astype(HALF)


def block(index, size):
    return pl.ds(pl.multiple_of(index * size, size), size)


def kernel(
    density_hbm,
    green_hbm,
    cas_hbm,
    out_ref,
    planes,
    green_in,
    cas,
    cas2,
    cas4,
    kron_f,
    kron_i,
    green_out,
    green_all,
    y_out,
    y_all,
    lhs_x,
    x_out,
    x_all,
    z_in,
    z_mid,
    z_out,
    z_all,
    rhs,
    i_out,
    i_all,
    lhs_y,
    part_i,
    load_sem,
    send_sem,
    recv_sem,
):
    me = {"gz": lax.axis_index("gz"), "pa": lax.axis_index("pa")}

    loads = [
        pltpu.make_async_copy(source, target, load_sem.at[i])
        for i, (source, target) in enumerate(
            ((green_hbm, green_in), (cas_hbm, cas), (density_hbm, planes))
        )
    ]
    for load in loads:
        load.start()

    barrier = pltpu.get_barrier_semaphore()
    for s in FAR_FIRST:
        for axis in ("gz", "pa"):
            pl.semaphore_signal(
                barrier, inc=1, device_id={axis: lax.rem(me[axis] + s, N)}, device_id_type=MESH
            )

    class Exchange:
        def __init__(self, number, axis, source, target):
            self.number, self.axis, self.source, self.target = number, axis, source, target

        def copy(self, peer):
            mine = me[self.axis]
            s = lax.rem(peer - mine + N, N)
            return pltpu.make_async_remote_copy(
                src_ref=self.source.at[peer],
                dst_ref=self.target.at[mine],
                send_sem=send_sem.at[self.number, s],
                recv_sem=recv_sem.at[self.number, s],
                device_id={self.axis: peer},
                device_id_type=MESH,
            )

        def arrive(self, peer):
            s = lax.rem(me[self.axis] - peer + N, N)
            pltpu.make_async_remote_copy(
                src_ref=self.source.at[peer],
                dst_ref=self.target.at[peer],
                send_sem=send_sem.at[self.number, s],
                recv_sem=recv_sem.at[self.number, s],
                device_id={self.axis: peer},
                device_id_type=MESH,
            ).wait_recv()

        def keep(self):
            mine = me[self.axis]
            self.target[mine] = self.source[mine]

        def send(self, steps=FAR_FIRST):
            for s in steps:
                self.copy(lax.rem(me[self.axis] + s, N)).start()

        def peer(self, turn, b):
            mine = me[self.axis]
            return 4 * lax.rem(mine // 4 + turn, 4) + lax.rem(lax.rem(mine, 4) + b, 4)

        def send_group(self, turn, own):
            if own:
                self.keep()
            for b in range(1 if own else 0, 4):
                self.copy(self.peer(turn, b)).start()

        def receive(self, steps=FAR_FIRST):
            for s in steps:
                self.arrive(lax.rem(me[self.axis] + s, N))

        def receive_group(self, turn):
            for b in range(0 if turn else 1, 4):
                self.arrive(self.peer(turn, b))

        def drain(self):
            for s in FAR_FIRST:
                self.copy(lax.rem(me[self.axis] + s, N)).wait_send()

    ex_y = Exchange(0, "pa", y_out, y_all)
    ex_green = [Exchange(1 + h, "gz", green_out.at[h], green_all.at[h]) for h in range(PARTS)]
    ex_x = [Exchange(3 + h, "gz", x_out.at[h], x_all.at[h]) for h in range(PARTS)]
    ex_z = [Exchange(5 + h, "gz", z_out.at[h], z_all.at[h]) for h in range(PARTS)]
    ex_i = [Exchange(7 + h, "pa", i_out.at[h], i_all.at[h]) for h in range(PARTS)]

    def y_forward():
        @pl.loop(0, 4)
        def _(j):
            value = dot_nt(cas[block(j, 256), :], planes[...]).astype(HALF)
            for i in range(4):
                y_out[4 * j + i] = value[64 * i : 64 * (i + 1), :]

    def green_narrow():
        @pl.loop(0, 8)
        def _(k):
            for u in range(8):
                value = green_in[k, :, 128 * u : 128 * (u + 1)].astype(HALF)
                for v in range(2):
                    for h in range(PARTS):
                        row = 32 * v + 16 * h
                        green_out[h, 2 * u + v, k] = value[row : row + 16]

    def tables():
        @pl.loop(0, N)
        def _(q):
            value = cas[block(q, 64), :]
            cas2[block(2 * q, 64), :] = value
            cas2[block(2 * q + 1, 64), :] = value
            for h in range(PARTS):
                for z in range(4):
                    for v in range(2):
                        row = 32 * v + 16 * h
                        cas4[h, block(q * 8 + z * 2 + v, 16), :] = value[row : row + 16]

        def spread(target, rows, cols):
            @pl.loop(0, rows // 16)
            def _(j):
                pick = 8 * ((iota((128, 1024), 0) >> 3) + 16 * j) == iota((128, 1024), 1)
                part = dot(one_hot(pick), cas[:, :128]).astype(HALF)
                wide = (iota((128, 8 * cols), 1) >> 3) == iota((128, 8 * cols), 0)
                full = dot(part, one_hot(wide))
                same = (iota((128, 8 * cols), 0) & 7) == (iota((128, 8 * cols), 1) & 7)
                target[block(j, 128), :] = jnp.where(same, full, 0.0).astype(HALF)

        spread(kron_f, 128, 64)
        spread(kron_i, 64, 128)

    lane = iota((64, 128), 1)

    def x_operand():
        masks = [one_hot((lane >> 6) == z) for z in range(2)]

        @pl.loop(0, N)
        def _(q):
            for z in range(4):
                part = y_all[q, :, 128 * (z // 2) : 128 * (z // 2 + 1)] * masks[z % 2]
                for h in range(PARTS):
                    for v in range(2):
                        row = 32 * v + 16 * h
                        to = 128 * h + 32 * z + 16 * v
                        lhs_x[to : to + 16, block(q, 128)] = part[row : row + 16]

    def x_forward(h):
        def group(turn, own):
            j = lax.rem(me["gz"] // 4 + turn, 4)
            value = dot(lhs_x[128 * h : 128 * (h + 1), :], cas2[:, block(j, 256)]).astype(HALF)
            for u in range(2):
                for v in range(2):
                    for z in range(4):
                        row = 32 * z + 16 * v
                        x_out[h, 4 * j + 2 * u + v, z] = value[
                            row : row + 16, 128 * u : 128 * (u + 1)
                        ]
            ex_x[h].send_group(turn, own)

        @pl.loop(1, 4)
        def _(turn):
            group(turn, False)

        group(0, True)

    def z_both(h):
        @pl.loop(0, N)
        def _(g):
            value = x_all[h, g].astype(jnp.float32)
            for v in range(2):
                part = value[:, 8 * v : 8 * v + 8, :].reshape(32, 128)
                z_in[block(g, 32), 128 * v : 128 * (v + 1)] = part.astype(HALF)

        @pl.loop(0, 4)
        def _(j):
            value = dot(kron_f[block(j, 256), :], z_in[...])
            for i in range(4):
                weight = green_all[h, 4 * j + i].astype(jnp.float32)
                for v in range(2):
                    part = weight[:, 8 * v : 8 * v + 8, :].reshape(64, 128)
                    part = part * value[64 * i : 64 * i + 64, 128 * v : 128 * (v + 1)]
                    z_mid[block(4 * j + i, 64), 128 * v : 128 * (v + 1)] = part.astype(HALF)

        @pl.loop(0, 2)
        def _(j):
            value = dot(kron_i[block(j, 256), :], z_mid[...])
            for b in range(8):
                part = value[32 * b : 32 * b + 32]
                part = jnp.concatenate(
                    [part[:, 128 * v : 128 * (v + 1)].reshape(4, 8, 128) for v in range(2)], axis=1
                )
                z_out[h, 8 * j + b] = part.astype(HALF)

        ex_z[h].send()
        ex_z[h].keep()

    def x_inverse(h):
        for last, turns in enumerate(((2, 1), (3, 0))):
            for turn in turns:
                ex_z[h].receive_group(turn)
            groups = [lax.rem(me["gz"] // 4 + turn, 4) for turn in turns]
            for t, j in enumerate(groups):
                for u in range(2):
                    for v in range(2):
                        for z in range(4):
                            row = 32 * z + 16 * v
                            column = 256 * t + 128 * u
                            rhs[last, row : row + 16, column : column + 128] = z_all[
                                h, 4 * j + 2 * u + v, z
                            ]
            for to in (1, 2, 3, 0):
                i = lax.rem(me["pa"] // 4 + to, 4)
                value = sum(
                    dot_nt(
                        cas[block(i, 256), block(j, 256)], rhs[last, :, 256 * t : 256 * (t + 1)]
                    )
                    for t, j in enumerate(groups)
                )
                if last:
                    value = (value + part_i[block(i, 256), :]).astype(HALF)
                    for b in range(4):
                        i_out[h, 4 * i + b] = value[64 * b : 64 * (b + 1), :]
                    ex_i[h].send_group(to, to == 0)
                else:
                    part_i[block(i, 256), :] = value

    masks = [one_hot((lane >> 5) == z) for z in range(4)]

    def y_inverse(h, steps):
        for step, turns in enumerate(steps):
            for turn in turns:
                ex_i[h].receive_group(turn)
            groups = [lax.rem(me["pa"] // 4 + turn, 4) for turn in turns]
            for i in groups:
                for b in range(4):
                    value = i_all[h, 4 * i + b]
                    for z in range(4):
                        lhs_y[64 * z : 64 * (z + 1), block(4 * i + b, 128)] = value * masks[z]
            for j in range(4):
                columns = slice(256 * j, 256 * (j + 1))
                value = sum(
                    dot(lhs_y[:, block(i, 512)], cas4[h, block(i, 512), columns]) for i in groups
                )
                if h or step:
                    value = value + out_ref[:, columns]
                out_ref[:, columns] = value

    scope = jax.named_scope
    with scope("load_green"):
        loads[0].wait()
    with scope("green_narrow"):
        green_narrow()
    with scope("load"):
        loads[1].wait()
        loads[2].wait()
    with scope("y_forward"):
        y_forward()
    with scope("barrier"):
        pl.semaphore_wait(barrier, 2 * (N - 1))
    with scope("send_y"):
        ex_green[0].send()
        ex_y.send()
        ex_green[1].send(FAR_FIRST[:7])
    with scope("tables"):
        ex_green[0].keep()
        ex_green[1].keep()
        ex_y.keep()
        tables()
    with scope("wait_y"):
        ex_y.receive()
    with scope("x_operand"):
        x_operand()
    with scope("x_forward0"):
        x_forward(0)
    with scope("send_green1"):
        ex_green[1].send(FAR_FIRST[7:])
    with scope("x_forward1"):
        x_forward(1)
    with scope("drain_early"):
        ex_y.drain()
        ex_green[0].drain()
    with scope("wait_green0"):
        ex_green[0].receive()
    with scope("wait_x0"):
        ex_x[0].receive()
    with scope("z_both0"):
        z_both(0)
    with scope("wait_green1"):
        ex_green[1].receive()
    with scope("drain_x0"):
        ex_x[0].drain()
    with scope("wait_x1"):
        ex_x[1].receive()
    with scope("z_both1"):
        z_both(1)
    with scope("drain_x1"):
        ex_green[1].drain()
        ex_x[1].drain()
    with scope("x_inverse0"):
        x_inverse(0)
    with scope("drain_z0"):
        ex_z[0].drain()
    with scope("x_inverse1"):
        x_inverse(1)
    with scope("y_inverse0"):
        y_inverse(0, ((0, 1, 3, 2),))
    with scope("drain_z1"):
        ex_z[1].drain()
        ex_i[0].drain()
    with scope("y_inverse1"):
        y_inverse(1, ((0, 1), (3,), (2,)))
    with scope("drain"):
        ex_i[1].drain()


def finish(scale, total, out_hbm, held, sem):
    rows = held.shape[0] // 4
    writes = [
        pltpu.make_async_copy(
            held.at[pl.ds(rows * i, rows)], out_hbm.at[pl.ds(rows * i, rows)], sem.at[i]
        )
        for i in range(4)
    ]
    for i, write in enumerate(writes):
        held[rows * i : rows * (i + 1), :] = total[rows * i : rows * (i + 1), :] * scale
        write.start()
    for write in writes:
        write.wait()


def solution(mesh):
    cas = cas_table(1024, 1024, 1024)
    scale = 1.0 / (1024 * 1024 * 128)

    def local(density, green, cas):
        def vmem(*shape, dtype=HALF):
            return pltpu.VMEM(shape, dtype)

        anywhere = pl.BlockSpec(memory_space=pl.ANY)
        near = pl.BlockSpec(memory_space=pltpu.VMEM)
        potential = pl.pallas_call(
            kernel,
            out_shape=jax.ShapeDtypeStruct((256, 1024), jnp.float32),
            in_specs=[anywhere, anywhere, anywhere],
            out_specs=near,
            scratch_shapes=[
                vmem(256, 1024),
                vmem(8, 64, 1024, dtype=jnp.float32),
                vmem(1024, 1024),
                vmem(2048, 1024),
                vmem(PARTS, 2048, 1024),
                vmem(1024, 512),
                vmem(512, 1024),
                vmem(PARTS, N, 8, 16, 128),
                vmem(PARTS, N, 8, 16, 128),
                vmem(N, 64, 256),
                vmem(N, 64, 256),
                vmem(256, 2048),
                vmem(PARTS, N, 4, 16, 128),
                vmem(PARTS, N, 4, 16, 128),
                vmem(512, 256),
                vmem(1024, 256),
                vmem(PARTS, N, 4, 16, 128),
                vmem(PARTS, N, 4, 16, 128),
                vmem(2, 128, 512),
                vmem(PARTS, N, 64, 128),
                vmem(PARTS, N, 64, 128),
                vmem(256, 2048),
                vmem(1024, 128, dtype=jnp.float32),
                pltpu.SemaphoreType.DMA((3,)),
                pltpu.SemaphoreType.DMA((9, N)),
                pltpu.SemaphoreType.DMA((9, N)),
            ],
            compiler_params=pltpu.CompilerParams(
                collective_id=0, has_side_effects=True, vmem_limit_bytes=48 * 1024 * 1024
            ),
            name="poisson",
        )(*[pltpu.with_memory_space_constraint(x, pltpu.HBM) for x in (density.reshape(256, 1024), green, cas)])
        potential = pl.pallas_call(
            lambda *refs: finish(scale, *refs),
            out_shape=jax.ShapeDtypeStruct((256, 1024), jnp.float32),
            in_specs=[near],
            out_specs=anywhere,
            scratch_shapes=[
                vmem(256, 1024, dtype=jnp.float32),
                pltpu.SemaphoreType.DMA((4,)),
            ],
            compiler_params=pltpu.CompilerParams(vmem_limit_bytes=8 * 1024 * 1024),
            name="finish",
        )(potential)
        return potential.reshape(4, 64, 1024)

    step = jax.shard_map(
        local,
        mesh=mesh,
        in_specs=(P("gz", "pa", None), P("gz", "pa", None), P()),
        out_specs=P("gz", "pa", None),
        check_vma=False,
    )
    return lambda density, green: step(density, green, cas)
```

```python
import math

import jax
import jax.numpy as jnp
import numpy as np
from jax import lax
from jax.experimental import pallas as pl
from jax.experimental.pallas import tpu as pltpu
from jax.sharding import PartitionSpec as P

MESH = pl.DeviceIdType.MESH
HALF = jnp.bfloat16
N = 16
PARTS = 2
FAR_FIRST = [8, 7, 9, 6, 10, 5, 11, 4, 12, 3, 13, 2, 14, 1, 15]


def cas_table(rows, cols, length):
    product = np.arange(rows)[:, None] * np.arange(cols)[None, :] % length
    angle = product.astype(np.float32) * np.float32(2.0 * math.pi / length)
    return jnp.asarray((np.cos(angle) + np.sin(angle)).astype(np.float32), HALF)


def dot(a, b):
    return jnp.dot(a, b, preferred_element_type=jnp.float32)


def dot_nt(a, b):
    return lax.dot_general(a, b, (((1,), (1,)), ((), ())), preferred_element_type=jnp.float32)


def iota(shape, dim):
    return lax.broadcasted_iota(jnp.int32, shape, dim)


def one_hot(condition):
    return condition.astype(jnp.float32).astype(HALF)


def block(index, size):
    return pl.ds(pl.multiple_of(index * size, size), size)


def kernel(
    scale,
    density_hbm,
    green_hbm,
    cas_hbm,
    out_ref,
    planes,
    green_in,
    cas,
    cas2,
    cas4,
    kron_f,
    kron_i,
    green_out,
    green_all,
    y_out,
    y_all,
    lhs_x,
    x_out,
    x_all,
    z_in,
    z_mid,
    z_out,
    z_all,
    rhs,
    i_out,
    i_all,
    lhs_y,
    part_i,
    load_sem,
    send_sem,
    recv_sem,
):
    me = {"gz": lax.axis_index("gz"), "pa": lax.axis_index("pa")}

    loads = [
        pltpu.make_async_copy(source, target, load_sem.at[i])
        for i, (source, target) in enumerate(
            ((green_hbm, green_in), (cas_hbm, cas), (density_hbm, planes))
        )
    ]
    for load in loads:
        load.start()

    barrier = pltpu.get_barrier_semaphore()
    for s in FAR_FIRST:
        for axis in ("gz", "pa"):
            pl.semaphore_signal(
                barrier, inc=1, device_id={axis: lax.rem(me[axis] + s, N)}, device_id_type=MESH
            )

    own = me["pa"] // 4
    pa_groups = [own, own + 1 - 2 * lax.rem(own, 2), lax.rem(own + 2, 4), 3 - own]

    class Exchange:
        def __init__(self, number, axis, source, target):
            self.number, self.axis, self.source, self.target = number, axis, source, target

        def copy(self, peer):
            mine = me[self.axis]
            s = lax.rem(peer - mine + N, N)
            return pltpu.make_async_remote_copy(
                src_ref=self.source.at[peer],
                dst_ref=self.target.at[mine],
                send_sem=send_sem.at[self.number, s],
                recv_sem=recv_sem.at[self.number, s],
                device_id={self.axis: peer},
                device_id_type=MESH,
            )

        def arrive(self, peer):
            s = lax.rem(me[self.axis] - peer + N, N)
            pltpu.make_async_remote_copy(
                src_ref=self.source.at[peer],
                dst_ref=self.target.at[peer],
                send_sem=send_sem.at[self.number, s],
                recv_sem=recv_sem.at[self.number, s],
                device_id={self.axis: peer},
                device_id_type=MESH,
            ).wait_recv()

        def keep(self):
            mine = me[self.axis]
            self.target[mine] = self.source[mine]

        def send(self, steps=FAR_FIRST):
            for s in steps:
                self.copy(lax.rem(me[self.axis] + s, N)).start()

        def peer(self, turn, b):
            mine = me[self.axis]
            if self.axis == "pa":
                group = pa_groups[turn]
            else:
                group = lax.rem(mine // 4 + turn, 4)
            return 4 * group + lax.rem(lax.rem(mine, 4) + b, 4)

        def send_group(self, turn, own):
            if own:
                self.keep()
            for b in range(1 if own else 0, 4):
                self.copy(self.peer(turn, b)).start()

        def receive(self, steps=FAR_FIRST):
            for s in steps:
                self.arrive(lax.rem(me[self.axis] + s, N))

        def receive_group(self, turn):
            for b in range(0 if turn else 1, 4):
                self.arrive(self.peer(turn, b))

        def drain(self):
            for s in FAR_FIRST:
                self.copy(lax.rem(me[self.axis] + s, N)).wait_send()

    ex_y = Exchange(0, "pa", y_out, y_all)
    ex_green = [Exchange(1 + h, "gz", green_out.at[h], green_all.at[h]) for h in range(PARTS)]
    ex_x = [Exchange(3 + h, "gz", x_out.at[h], x_all.at[h]) for h in range(PARTS)]
    ex_z = [Exchange(5 + h, "gz", z_out.at[h], z_all.at[h]) for h in range(PARTS)]
    ex_i = [Exchange(7 + h, "pa", i_out.at[h], i_all.at[h]) for h in range(PARTS)]

    def y_forward():
        @pl.loop(0, 4)
        def _(j):
            value = dot_nt(cas[block(j, 256), :], planes[...]).astype(HALF)
            for i in range(4):
                y_out[4 * j + i] = value[64 * i : 64 * (i + 1), :]

    def green_narrow():
        @pl.loop(0, 8)
        def _(k):
            for u in range(8):
                value = green_in[k, :, 128 * u : 128 * (u + 1)].astype(HALF)
                for v in range(2):
                    for h in range(PARTS):
                        row = 32 * v + 16 * h
                        green_out[h, 2 * u + v, k] = value[row : row + 16]

    def tables():
        @pl.loop(0, N)
        def _(q):
            value = cas[block(q, 64), :]
            cas2[block(2 * q, 64), :] = value
            cas2[block(2 * q + 1, 64), :] = value
            for h in range(PARTS):
                for z in range(4):
                    for v in range(2):
                        row = 32 * v + 16 * h
                        cas4[h, block(q * 8 + z * 2 + v, 16), :] = value[row : row + 16]

        def spread(target, rows, cols):
            @pl.loop(0, rows // 16)
            def _(j):
                pick = 8 * ((iota((128, 1024), 0) >> 3) + 16 * j) == iota((128, 1024), 1)
                part = dot(one_hot(pick), cas[:, :128]).astype(HALF)
                wide = (iota((128, 8 * cols), 1) >> 3) == iota((128, 8 * cols), 0)
                full = dot(part, one_hot(wide))
                same = (iota((128, 8 * cols), 0) & 7) == (iota((128, 8 * cols), 1) & 7)
                target[block(j, 128), :] = jnp.where(same, full, 0.0).astype(HALF)

        spread(kron_f, 128, 64)
        spread(kron_i, 64, 128)

    lane = iota((64, 128), 1)

    def x_operand():
        masks = [one_hot((lane >> 6) == z) for z in range(2)]

        @pl.loop(0, N)
        def _(q):
            for z in range(4):
                part = y_all[q, :, 128 * (z // 2) : 128 * (z // 2 + 1)] * masks[z % 2]
                for h in range(PARTS):
                    for v in range(2):
                        row = 32 * v + 16 * h
                        to = 128 * h + 32 * z + 16 * v
                        lhs_x[to : to + 16, block(q, 128)] = part[row : row + 16]

    def x_forward(h):
        def group(turn, own):
            j = lax.rem(me["gz"] // 4 + turn, 4)
            value = dot(lhs_x[128 * h : 128 * (h + 1), :], cas2[:, block(j, 256)]).astype(HALF)
            for u in range(2):
                for v in range(2):
                    for z in range(4):
                        row = 32 * z + 16 * v
                        x_out[h, 4 * j + 2 * u + v, z] = value[
                            row : row + 16, 128 * u : 128 * (u + 1)
                        ]
            ex_x[h].send_group(turn, own)

        @pl.loop(1, 4)
        def _(turn):
            group(turn, False)

        group(0, True)

    def z_both(h):
        @pl.loop(0, N)
        def _(g):
            value = x_all[h, g].astype(jnp.float32)
            for v in range(2):
                part = value[:, 8 * v : 8 * v + 8, :].reshape(32, 128)
                z_in[block(g, 32), 128 * v : 128 * (v + 1)] = part.astype(HALF)

        @pl.loop(0, 4)
        def _(j):
            value = dot(kron_f[block(j, 256), :], z_in[...])
            for i in range(4):
                weight = green_all[h, 4 * j + i].astype(jnp.float32)
                for v in range(2):
                    part = weight[:, 8 * v : 8 * v + 8, :].reshape(64, 128)
                    part = part * value[64 * i : 64 * i + 64, 128 * v : 128 * (v + 1)]
                    z_mid[block(4 * j + i, 64), 128 * v : 128 * (v + 1)] = part.astype(HALF)

        @pl.loop(0, 2)
        def _(j):
            value = dot(kron_i[block(j, 256), :], z_mid[...])
            for b in range(8):
                part = value[32 * b : 32 * b + 32]
                part = jnp.concatenate(
                    [part[:, 128 * v : 128 * (v + 1)].reshape(4, 8, 128) for v in range(2)], axis=1
                )
                z_out[h, 8 * j + b] = part.astype(HALF)

        ex_z[h].send()
        ex_z[h].keep()

    def x_inverse(h):
        for last, turns in enumerate(((2, 1), (3, 0))):
            for turn in turns:
                ex_z[h].receive_group(turn)
            groups = [lax.rem(me["gz"] // 4 + turn, 4) for turn in turns]
            for t, j in enumerate(groups):
                for u in range(2):
                    for v in range(2):
                        for z in range(4):
                            row = 32 * z + 16 * v
                            column = 256 * t + 128 * u
                            rhs[last, row : row + 16, column : column + 128] = z_all[
                                h, 4 * j + 2 * u + v, z
                            ]
            for turn in (3, 2, 1, 0):
                i = pa_groups[turn]
                value = sum(
                    dot_nt(
                        cas[block(i, 256), block(j, 256)], rhs[last, :, 256 * t : 256 * (t + 1)]
                    )
                    for t, j in enumerate(groups)
                )
                if last:
                    value = (value + part_i[block(i, 256), :]).astype(HALF)
                    for b in range(4):
                        i_out[h, 4 * i + b] = value[64 * b : 64 * (b + 1), :]
                    ex_i[h].send_group(turn, turn == 0)
                else:
                    part_i[block(i, 256), :] = value

    masks = [one_hot((lane >> 5) == z) for z in range(4)]

    def y_inverse(h, steps):
        for step, turns in enumerate(steps):
            for turn in turns:
                ex_i[h].receive_group(turn)
            groups = [pa_groups[turn] for turn in turns]
            for i in groups:
                for b in range(4):
                    value = i_all[h, 4 * i + b]
                    for z in range(4):
                        lhs_y[64 * z : 64 * (z + 1), block(4 * i + b, 128)] = value * masks[z]
            for j in range(4):
                columns = slice(256 * j, 256 * (j + 1))
                value = sum(
                    dot(lhs_y[:, block(i, 512)], cas4[h, block(i, 512), columns]) for i in groups
                )
                if h or step:
                    value = value + out_ref[:, columns]
                if h == PARTS - 1 and step == len(steps) - 1:
                    value = value * scale
                out_ref[:, columns] = value

    scope = jax.named_scope
    with scope("load_green"):
        loads[0].wait()
    with scope("green_narrow"):
        green_narrow()
    with scope("load"):
        loads[1].wait()
        loads[2].wait()
    with scope("y_forward"):
        y_forward()
    with scope("barrier"):
        pl.semaphore_wait(barrier, 2 * (N - 1))
    with scope("send_y"):
        ex_green[0].send()
        ex_y.send()
        ex_green[1].send(FAR_FIRST[:7])
    with scope("tables"):
        ex_green[0].keep()
        ex_green[1].keep()
        ex_y.keep()
        tables()
    with scope("wait_y"):
        ex_y.receive()
    with scope("x_operand"):
        x_operand()
    with scope("x_forward0"):
        x_forward(0)
    with scope("send_green1"):
        ex_green[1].send(FAR_FIRST[7:])
    with scope("x_forward1"):
        x_forward(1)
    with scope("drain_early"):
        ex_y.drain()
        ex_green[0].drain()
    with scope("wait_green0"):
        ex_green[0].receive()
    with scope("wait_x0"):
        ex_x[0].receive()
    with scope("z_both0"):
        z_both(0)
    with scope("wait_green1"):
        ex_green[1].receive()
    with scope("drain_x0"):
        ex_x[0].drain()
    with scope("wait_x1"):
        ex_x[1].receive()
    with scope("z_both1"):
        z_both(1)
    with scope("drain_x1"):
        ex_green[1].drain()
        ex_x[1].drain()
    with scope("x_inverse0"):
        x_inverse(0)
    with scope("drain_z0"):
        ex_z[0].drain()
    with scope("x_inverse1"):
        x_inverse(1)
    with scope("y_inverse0"):
        y_inverse(0, ((0, 1, 2, 3),))
    with scope("drain_z1"):
        ex_z[1].drain()
        ex_i[0].drain()
    with scope("y_inverse1"):
        y_inverse(1, ((0, 1), (2,), (3,)))
    with scope("drain"):
        ex_i[1].drain()


def finish(total, out_hbm, sem):
    write = pltpu.make_async_copy(total, out_hbm, sem)
    write.start()
    write.wait()


def solution(mesh):
    cas = cas_table(1024, 1024, 1024)
    scale = 1.0 / (1024 * 1024 * 128)

    def local(density, green, cas):
        def vmem(*shape, dtype=HALF):
            return pltpu.VMEM(shape, dtype)

        anywhere = pl.BlockSpec(memory_space=pl.ANY)
        near = pl.BlockSpec(memory_space=pltpu.VMEM)
        potential = pl.pallas_call(
            lambda *refs: kernel(scale, *refs),
            out_shape=jax.ShapeDtypeStruct((256, 1024), jnp.float32),
            in_specs=[anywhere, anywhere, anywhere],
            out_specs=near,
            scratch_shapes=[
                vmem(256, 1024),
                vmem(8, 64, 1024, dtype=jnp.float32),
                vmem(1024, 1024),
                vmem(2048, 1024),
                vmem(PARTS, 2048, 1024),
                vmem(1024, 512),
                vmem(512, 1024),
                vmem(PARTS, N, 8, 16, 128),
                vmem(PARTS, N, 8, 16, 128),
                vmem(N, 64, 256),
                vmem(N, 64, 256),
                vmem(256, 2048),
                vmem(PARTS, N, 4, 16, 128),
                vmem(PARTS, N, 4, 16, 128),
                vmem(512, 256),
                vmem(1024, 256),
                vmem(PARTS, N, 4, 16, 128),
                vmem(PARTS, N, 4, 16, 128),
                vmem(2, 128, 512),
                vmem(PARTS, N, 64, 128),
                vmem(PARTS, N, 64, 128),
                vmem(256, 2048),
                vmem(1024, 128, dtype=jnp.float32),
                pltpu.SemaphoreType.DMA((3,)),
                pltpu.SemaphoreType.DMA((9, N)),
                pltpu.SemaphoreType.DMA((9, N)),
            ],
            compiler_params=pltpu.CompilerParams(
                collective_id=0, has_side_effects=True, vmem_limit_bytes=48 * 1024 * 1024
            ),
            name="poisson",
        )(*[pltpu.with_memory_space_constraint(x, pltpu.HBM) for x in (density.reshape(256, 1024), green, cas)])
        potential = pl.pallas_call(
            finish,
            out_shape=jax.ShapeDtypeStruct((256, 1024), jnp.float32),
            in_specs=[near],
            out_specs=anywhere,
            scratch_shapes=[pltpu.SemaphoreType.DMA(())],
            compiler_params=pltpu.CompilerParams(vmem_limit_bytes=8 * 1024 * 1024),
            name="finish",
        )(potential)
        return potential.reshape(4, 64, 1024)

    step = jax.shard_map(
        local,
        mesh=mesh,
        in_specs=(P("gz", "pa", None), P("gz", "pa", None), P()),
        out_specs=P("gz", "pa", None),
        check_vma=False,
    )
    return lambda density, green: step(density, green, cas)
```

```python
import math

import jax
import jax.numpy as jnp
import numpy as np
from jax import lax
from jax.experimental import pallas as pl
from jax.experimental.pallas import tpu as pltpu
from jax.sharding import PartitionSpec as P

MESH = pl.DeviceIdType.MESH
HALF = jnp.bfloat16
N = 16
PARTS = 2
FAR_FIRST = [8, 7, 9, 6, 10, 5, 11, 4, 12, 3, 13, 2, 14, 1, 15]


def cas_table(rows, cols, length):
    product = np.arange(rows)[:, None] * np.arange(cols)[None, :] % length
    angle = product.astype(np.float32) * np.float32(2.0 * math.pi / length)
    return jnp.asarray((np.cos(angle) + np.sin(angle)).astype(np.float32), HALF)


def dot(a, b):
    return jnp.dot(a, b, preferred_element_type=jnp.float32)


def dot_nt(a, b):
    return lax.dot_general(a, b, (((1,), (1,)), ((), ())), preferred_element_type=jnp.float32)


def iota(shape, dim):
    return lax.broadcasted_iota(jnp.int32, shape, dim)


def one_hot(condition):
    return condition.astype(jnp.float32).astype(HALF)


def block(index, size):
    return pl.ds(pl.multiple_of(index * size, size), size)


def kernel(
    scale,
    density_hbm,
    green_hbm,
    cas_hbm,
    out_ref,
    planes,
    green_in,
    cas,
    cas2,
    cas4,
    kron_f,
    kron_i,
    green_out,
    green_all,
    y_out,
    y_all,
    lhs_x,
    x_out,
    x_all,
    z_in,
    z_mid,
    z_out,
    z_all,
    rhs,
    i_out,
    i_all,
    lhs_y,
    part_i,
    load_sem,
    send_sem,
    recv_sem,
):
    me = {"gz": lax.axis_index("gz"), "pa": lax.axis_index("pa")}

    loads = [
        pltpu.make_async_copy(source, target, load_sem.at[i])
        for i, (source, target) in enumerate(
            ((green_hbm, green_in), (cas_hbm, cas), (density_hbm, planes))
        )
    ]
    for load in loads:
        load.start()

    barrier = pltpu.get_barrier_semaphore()
    for s in FAR_FIRST:
        for axis in ("gz", "pa"):
            pl.semaphore_signal(
                barrier, inc=1, device_id={axis: lax.rem(me[axis] + s, N)}, device_id_type=MESH
            )

    own = me["pa"] // 4
    pa_groups = [own, own + 1 - 2 * lax.rem(own, 2), lax.rem(own + 2, 4), 3 - own]

    class Exchange:
        def __init__(self, number, axis, source, target):
            self.number, self.axis, self.source, self.target = number, axis, source, target

        def copy(self, peer):
            mine = me[self.axis]
            s = lax.rem(peer - mine + N, N)
            return pltpu.make_async_remote_copy(
                src_ref=self.source.at[peer],
                dst_ref=self.target.at[mine],
                send_sem=send_sem.at[self.number, s],
                recv_sem=recv_sem.at[self.number, s],
                device_id={self.axis: peer},
                device_id_type=MESH,
            )

        def arrive(self, peer):
            s = lax.rem(me[self.axis] - peer + N, N)
            pltpu.make_async_remote_copy(
                src_ref=self.source.at[peer],
                dst_ref=self.target.at[peer],
                send_sem=send_sem.at[self.number, s],
                recv_sem=recv_sem.at[self.number, s],
                device_id={self.axis: peer},
                device_id_type=MESH,
            ).wait_recv()

        def keep(self):
            mine = me[self.axis]
            self.target[mine] = self.source[mine]

        def send(self, steps=FAR_FIRST):
            for s in steps:
                self.copy(lax.rem(me[self.axis] + s, N)).start()

        def peer(self, turn, b):
            mine = me[self.axis]
            if self.axis == "pa":
                group = pa_groups[turn]
            else:
                group = lax.rem(mine // 4 + turn, 4)
            return 4 * group + lax.rem(lax.rem(mine, 4) + b, 4)

        def send_group(self, turn, own):
            if own:
                self.keep()
            for b in range(1 if own else 0, 4):
                self.copy(self.peer(turn, b)).start()

        def receive(self, steps=FAR_FIRST):
            for s in steps:
                self.arrive(lax.rem(me[self.axis] + s, N))

        def receive_group(self, turn):
            for b in range(0 if turn else 1, 4):
                self.arrive(self.peer(turn, b))

        def drain(self):
            for s in FAR_FIRST:
                self.copy(lax.rem(me[self.axis] + s, N)).wait_send()

    ex_y = Exchange(0, "pa", y_out, y_all)
    ex_green = [Exchange(1 + h, "gz", green_out.at[h], green_all.at[h]) for h in range(PARTS)]
    ex_x = [Exchange(3 + h, "gz", x_out.at[h], x_all.at[h]) for h in range(PARTS)]
    ex_z = [Exchange(5 + h, "gz", z_out.at[h], z_all.at[h]) for h in range(PARTS)]
    ex_i = [Exchange(7 + h, "pa", i_out.at[h], i_all.at[h]) for h in range(PARTS)]

    def y_forward():
        @pl.loop(0, 4)
        def _(j):
            value = dot_nt(cas[block(j, 256), :], planes[...]).astype(HALF)
            for i in range(4):
                y_out[4 * j + i] = value[64 * i : 64 * (i + 1), :]

    def green_narrow():
        @pl.loop(0, 8)
        def _(k):
            for u in range(8):
                value = green_in[k, :, 128 * u : 128 * (u + 1)].astype(HALF)
                for v in range(2):
                    for h in range(PARTS):
                        row = 32 * v + 16 * h
                        green_out[h, 2 * u + v, k] = value[row : row + 16]

    def tables():
        @pl.loop(0, N)
        def _(q):
            value = cas[block(q, 64), :]
            cas2[block(2 * q, 64), :] = value
            cas2[block(2 * q + 1, 64), :] = value
            for h in range(PARTS):
                for z in range(4):
                    for v in range(2):
                        row = 32 * v + 16 * h
                        cas4[h, block(q * 8 + z * 2 + v, 16), :] = value[row : row + 16]

        def spread(target, rows, cols):
            @pl.loop(0, rows // 16)
            def _(j):
                pick = 8 * ((iota((128, 1024), 0) >> 3) + 16 * j) == iota((128, 1024), 1)
                part = dot(one_hot(pick), cas[:, :128]).astype(HALF)
                wide = (iota((128, 8 * cols), 1) >> 3) == iota((128, 8 * cols), 0)
                full = dot(part, one_hot(wide))
                same = (iota((128, 8 * cols), 0) & 7) == (iota((128, 8 * cols), 1) & 7)
                target[block(j, 128), :] = jnp.where(same, full, 0.0).astype(HALF)

        spread(kron_f, 128, 64)
        spread(kron_i, 64, 128)

    lane = iota((64, 128), 1)

    def x_operand():
        masks = [one_hot((lane >> 6) == z) for z in range(2)]

        @pl.loop(0, N)
        def _(q):
            for z in range(4):
                part = y_all[q, :, 128 * (z // 2) : 128 * (z // 2 + 1)] * masks[z % 2]
                for h in range(PARTS):
                    for v in range(2):
                        row = 32 * v + 16 * h
                        to = 128 * h + 32 * z + 16 * v
                        lhs_x[to : to + 16, block(q, 128)] = part[row : row + 16]

    def x_forward(h):
        def group(turn, own):
            j = lax.rem(me["gz"] // 4 + turn, 4)
            value = dot(lhs_x[128 * h : 128 * (h + 1), :], cas2[:, block(j, 256)]).astype(HALF)
            for u in range(2):
                for v in range(2):
                    for z in range(4):
                        row = 32 * z + 16 * v
                        x_out[h, 4 * j + 2 * u + v, z] = value[
                            row : row + 16, 128 * u : 128 * (u + 1)
                        ]
            ex_x[h].send_group(turn, own)

        @pl.loop(1, 4)
        def _(turn):
            group(turn, False)

        group(0, True)

    def z_both(h):
        @pl.loop(0, N)
        def _(g):
            value = x_all[h, g].astype(jnp.float32)
            for v in range(2):
                part = value[:, 8 * v : 8 * v + 8, :].reshape(32, 128)
                z_in[block(g, 32), 128 * v : 128 * (v + 1)] = part.astype(HALF)

        @pl.loop(0, 4)
        def _(j):
            value = dot(kron_f[block(j, 256), :], z_in[...])
            for i in range(4):
                weight = green_all[h, 4 * j + i].astype(jnp.float32)
                for v in range(2):
                    part = weight[:, 8 * v : 8 * v + 8, :].reshape(64, 128)
                    part = part * value[64 * i : 64 * i + 64, 128 * v : 128 * (v + 1)]
                    z_mid[block(4 * j + i, 64), 128 * v : 128 * (v + 1)] = part.astype(HALF)

        for near in range(2):
            j = lax.rem(me["gz"] // 8 + 1 - near, 2)
            value = dot(kron_i[block(j, 256), :], z_mid[...])
            for b in range(8):
                part = value[32 * b : 32 * b + 32]
                part = jnp.concatenate(
                    [part[:, 128 * v : 128 * (v + 1)].reshape(4, 8, 128) for v in range(2)], axis=1
                )
                z_out[h, 8 * j + b] = part.astype(HALF)

            if near:
                ex_z[h].keep()
            for b in range(near, 8):
                ex_z[h].copy(8 * j + lax.rem(lax.rem(me["gz"], 8) + b, 8)).start()

    def x_inverse(h):
        for last, turns in enumerate(((2, 1), (3, 0))):
            for turn in turns:
                ex_z[h].receive_group(turn)
            groups = [lax.rem(me["gz"] // 4 + turn, 4) for turn in turns]
            for t, j in enumerate(groups):
                for u in range(2):
                    for v in range(2):
                        for z in range(4):
                            row = 32 * z + 16 * v
                            column = 256 * t + 128 * u
                            rhs[last, row : row + 16, column : column + 128] = z_all[
                                h, 4 * j + 2 * u + v, z
                            ]
            for turn in (3, 2, 1, 0):
                i = pa_groups[turn]
                value = sum(
                    dot_nt(
                        cas[block(i, 256), block(j, 256)], rhs[last, :, 256 * t : 256 * (t + 1)]
                    )
                    for t, j in enumerate(groups)
                )
                if last:
                    value = (value + part_i[block(i, 256), :]).astype(HALF)
                    for b in range(4):
                        i_out[h, 4 * i + b] = value[64 * b : 64 * (b + 1), :]
                    ex_i[h].send_group(turn, turn == 0)
                else:
                    part_i[block(i, 256), :] = value

    masks = [one_hot((lane >> 5) == z) for z in range(4)]

    def y_inverse(h, steps):
        for step, turns in enumerate(steps):
            for turn in turns:
                ex_i[h].receive_group(turn)
            groups = [pa_groups[turn] for turn in turns]
            for i in groups:
                for b in range(4):
                    value = i_all[h, 4 * i + b]
                    for z in range(4):
                        lhs_y[64 * z : 64 * (z + 1), block(4 * i + b, 128)] = value * masks[z]
            for j in range(4):
                columns = slice(256 * j, 256 * (j + 1))
                value = sum(
                    dot(lhs_y[:, block(i, 512)], cas4[h, block(i, 512), columns]) for i in groups
                )
                if h or step:
                    value = value + out_ref[:, columns]
                if h == PARTS - 1 and step == len(steps) - 1:
                    value = value * scale
                out_ref[:, columns] = value

    scope = jax.named_scope
    with scope("load_green"):
        loads[0].wait()
    with scope("green_narrow"):
        green_narrow()
    with scope("load"):
        loads[1].wait()
        loads[2].wait()
    with scope("y_forward"):
        y_forward()
    with scope("barrier"):
        pl.semaphore_wait(barrier, 2 * (N - 1))
    with scope("send_y"):
        ex_green[0].send()
        ex_y.send()
        ex_green[1].send(FAR_FIRST[:7])
    with scope("tables"):
        ex_green[0].keep()
        ex_green[1].keep()
        ex_y.keep()
        tables()
    with scope("wait_y"):
        ex_y.receive()
    with scope("x_operand"):
        x_operand()
    with scope("x_forward0"):
        x_forward(0)
    with scope("send_green1"):
        ex_green[1].send(FAR_FIRST[7:])
    with scope("x_forward1"):
        x_forward(1)
    with scope("drain_early"):
        ex_y.drain()
        ex_green[0].drain()
    with scope("wait_green0"):
        ex_green[0].receive()
    with scope("wait_x0"):
        ex_x[0].receive()
    with scope("z_both0"):
        z_both(0)
    with scope("wait_green1"):
        ex_green[1].receive()
    with scope("drain_x0"):
        ex_x[0].drain()
    with scope("wait_x1"):
        ex_x[1].receive()
    with scope("z_both1"):
        z_both(1)
    with scope("drain_x1"):
        ex_green[1].drain()
        ex_x[1].drain()
    with scope("x_inverse0"):
        x_inverse(0)
    with scope("drain_z0"):
        ex_z[0].drain()
    with scope("x_inverse1"):
        x_inverse(1)
    with scope("y_inverse0"):
        y_inverse(0, ((0, 1, 2, 3),))
    with scope("drain_z1"):
        ex_z[1].drain()
        ex_i[0].drain()
    with scope("y_inverse1"):
        y_inverse(1, ((0, 1), (2,), (3,)))
    with scope("drain"):
        ex_i[1].drain()


def finish(total, out_hbm, sem):
    write = pltpu.make_async_copy(total, out_hbm, sem)
    write.start()
    write.wait()


def solution(mesh):
    cas = cas_table(1024, 1024, 1024)
    scale = 1.0 / (1024 * 1024 * 128)

    def local(density, green, cas):
        def vmem(*shape, dtype=HALF):
            return pltpu.VMEM(shape, dtype)

        anywhere = pl.BlockSpec(memory_space=pl.ANY)
        near = pl.BlockSpec(memory_space=pltpu.VMEM)
        potential = pl.pallas_call(
            lambda *refs: kernel(scale, *refs),
            out_shape=jax.ShapeDtypeStruct((256, 1024), jnp.float32),
            in_specs=[anywhere, anywhere, anywhere],
            out_specs=near,
            scratch_shapes=[
                vmem(256, 1024),
                vmem(8, 64, 1024, dtype=jnp.float32),
                vmem(1024, 1024),
                vmem(2048, 1024),
                vmem(PARTS, 2048, 1024),
                vmem(1024, 512),
                vmem(512, 1024),
                vmem(PARTS, N, 8, 16, 128),
                vmem(PARTS, N, 8, 16, 128),
                vmem(N, 64, 256),
                vmem(N, 64, 256),
                vmem(256, 2048),
                vmem(PARTS, N, 4, 16, 128),
                vmem(PARTS, N, 4, 16, 128),
                vmem(512, 256),
                vmem(1024, 256),
                vmem(PARTS, N, 4, 16, 128),
                vmem(PARTS, N, 4, 16, 128),
                vmem(2, 128, 512),
                vmem(PARTS, N, 64, 128),
                vmem(PARTS, N, 64, 128),
                vmem(256, 2048),
                vmem(1024, 128, dtype=jnp.float32),
                pltpu.SemaphoreType.DMA((3,)),
                pltpu.SemaphoreType.DMA((9, N)),
                pltpu.SemaphoreType.DMA((9, N)),
            ],
            compiler_params=pltpu.CompilerParams(
                collective_id=0, has_side_effects=True, vmem_limit_bytes=48 * 1024 * 1024
            ),
            name="poisson",
        )(*[pltpu.with_memory_space_constraint(x, pltpu.HBM) for x in (density.reshape(256, 1024), green, cas)])
        potential = pl.pallas_call(
            finish,
            out_shape=jax.ShapeDtypeStruct((256, 1024), jnp.float32),
            in_specs=[near],
            out_specs=anywhere,
            scratch_shapes=[pltpu.SemaphoreType.DMA(())],
            compiler_params=pltpu.CompilerParams(vmem_limit_bytes=8 * 1024 * 1024),
            name="finish",
        )(potential)
        return potential.reshape(4, 64, 1024)

    step = jax.shard_map(
        local,
        mesh=mesh,
        in_specs=(P("gz", "pa", None), P("gz", "pa", None), P()),
        out_specs=P("gz", "pa", None),
        check_vma=False,
    )
    return lambda density, green: step(density, green, cas)
```
